32 devices in a mesh: gx: 4 (over x, core), gy: 2 (over y), gz: 4 (over z).
Axes of the slice: x: 2, y: 2, z: 4, core: 2. Of those that a mesh axis runs over, the one named last changes fastest.
Arguments:
- grid_inputs: bfloat16 [186, 256, 256], P(None, 'gx', 'gy'), may hold values from -6 to 6
- embed_w1: bfloat16 [512, 186], replicated, may hold values from -0.4375 to 0.4375
- embed_b1: float32 [512], replicated, may hold values from -3 to 3
- embed_w2: bfloat16 [512, 512], replicated, may hold values from -0.25 to 0.25
- embed_gain: float32 [512], replicated, may hold values from 0.1 to 1.9
- edge_w1: bfloat16 [512, 1536], replicated, may hold values from -0.15625 to 0.15625
- edge_b1: float32 [512], replicated, may hold values from -3 to 3
- edge_w2: bfloat16 [512, 512], replicated, may hold values from -0.25 to 0.25
- message_gain: float32 [512], replicated, may hold values from 0.1 to 1.9
- message_bias: float32 [512], replicated, may hold values from -3 to 3
- mesh_latent: bfloat16 [512, 4, 2, 256], P('gz', 'gx', 'gy'), may hold values from -6 to 6
- edge_latent: bfloat16 [512, 4, 2, 2048], P('gz', 'gx', 'gy'), may hold values from -6 to 6
- senders: int32 [4, 2, 2048], P('gx', 'gy'), may hold values from 0 to 65535, as said below
- receivers: int32 [4, 2, 2048], P('gx', 'gy'), may hold values from 0 to 2047, as said below
- edge_counts: int32 [4, 2], P('gx', 'gy'), may hold values from 1 to 2048, as said below
Outputs:
- mesh_out: bfloat16 [512, 4, 2, 256], P('gz', 'gx', 'gy')
- grid_latent: bfloat16 [512, 256, 256], P('gz', 'gx', 'gy')
The draws below stay inside these ranges and needn't reach their ends.
Inputs may be any that keep to these rules, and one draw needn't show every extreme that they name: `senders`: an edge of tile (b, c) has its sender's row within 8 rows of rows b * 64 to (b + 1) * 64 - 1, clipped to the grid, and its column within 8 columns, cyclically, of columns c * 128 to (c + 1) * 128 - 1; this holds in every slot. `receivers`: an edge of tile t is received by a node of that tile, t * 256 to (t + 1) * 256 - 1, in every slot. `edge_counts`: the live edges of a tile are its first slots; some tile holds 2048 live edges.
All inputs are finite; a program needn't handle non-finite values.
Results may differ from the reference program's by a relative error of at most 0.0049.
Values may be sent and summed in bfloat16 or wider, within the bound.
A program may use at most 128 MiB of HBM per device.

```python
import jax
import jax.numpy as jnp
from jax import lax

LATENT = 512
CHANNELS = 186
GLAT = 64
GLON = 128
MESH_DEV = 256
EDGE_DEV = 2048
HALO = 8
BANDS = 4
SECTORS = 2
NLAT = 256
NLON = 256


def tile_coords():
    band_ids = jnp.arange(BANDS, dtype=jnp.int32)[:, None, None]
    sector_ids = jnp.arange(SECTORS, dtype=jnp.int32)[None, :, None]
    return (band_ids, sector_ids)


def draw_senders(key, part):
    band_ids, sector_ids = tile_coords()
    lat_key, lon_key = jax.random.split(jax.random.fold_in(key, 11))
    shape = (BANDS, SECTORS, EDGE_DEV)
    rows = jax.random.randint(lat_key, shape, 0, GLAT + 2 * HALO, dtype=jnp.int32) + band_ids * GLAT - HALO
    rows = jnp.clip(rows, 0, NLAT - 1)
    columns = jax.random.randint(lon_key, shape, 0, GLON + 2 * HALO, dtype=jnp.int32) + sector_ids * GLON - HALO + NLON
    columns = columns % NLON
    return (rows * NLON + columns).astype(jnp.int32)


def draw_receivers(key, part):
    band_ids, sector_ids = tile_coords()
    first_key, second_key = jax.random.split(jax.random.fold_in(key, 23))
    shape = (BANDS, SECTORS, EDGE_DEV)
    first = jax.random.randint(first_key, shape, 0, MESH_DEV, dtype=jnp.int32)
    second = jax.random.randint(second_key, shape, 0, MESH_DEV, dtype=jnp.int32)
    return ((band_ids * SECTORS + sector_ids) * MESH_DEV + jnp.minimum(first, second)).astype(jnp.int32)


def draw_edge_counts(key, part):
    band_ids = jnp.arange(BANDS, dtype=jnp.int32)[:, None]
    sector_ids = jnp.arange(SECTORS, dtype=jnp.int32)[None, :]
    distance = jnp.abs(2 * band_ids + 1 - BANDS)
    base = EDGE_DEV // 8 + (EDGE_DEV - EDGE_DEV // 8) * (distance - 1) * (distance - 1) // ((BANDS - 2) * (BANDS - 2))
    jitter_key, pick_key = jax.random.split(jax.random.fold_in(key, 37))
    jitter = jax.random.randint(jitter_key, (BANDS, SECTORS), 0, EDGE_DEV // 64 + 1, dtype=jnp.int32)
    chosen = jax.random.randint(pick_key, (BANDS, 1), 0, SECTORS, dtype=jnp.int32)
    jitter = jnp.where((distance == BANDS - 1) & (sector_ids == chosen), 0, jitter)
    return (base - jitter).astype(jnp.int32)


def steps_of(rng, dims, shards, smallest, top_value):
    loudness = 1.0
    for dim, blocks in shards:
        steps = jax.random.uniform(jax.random.fold_in(jax.random.fold_in(rng, 6), dim), (blocks,), jnp.float32, smallest / len(shards), top_value / len(shards))
        loudness = loudness * jnp.repeat(jnp.exp(steps), dims[dim] // blocks).reshape((-1,) + (1,) * (len(dims) - 1 - dim))
    return loudness


def normal_values(stream_key, dims, width, reach, cuts=(), kind=jnp.bfloat16):
    values = width * jax.random.normal(stream_key, dims, jnp.float32)
    if cuts:
        values = values * steps_of(stream_key, dims, cuts, -0.22, 0.18)
    return jnp.clip(values, -reach, reach).astype(kind)


def setup_inputs(seed: int = 0) -> dict:
    keys = jax.random.split(jax.random.key(seed), 16)
    return {
        "grid_inputs": normal_values(keys[0], (CHANNELS, NLAT, NLON), 1.0, 6.0, ((1, 4), (2, 2))),
        "embed_w1": normal_values(keys[1], (LATENT, CHANNELS), CHANNELS ** -0.5, 0.4375),
        "embed_b1": normal_values(keys[2], (LATENT,), 0.5, 3.0, (), jnp.float32),
        "embed_w2": normal_values(keys[3], (LATENT, LATENT), LATENT ** -0.5, 0.25),
        "embed_gain": jnp.clip(1.0 + 0.18 * jax.random.normal(keys[4], (LATENT,), jnp.float32), 0.1, 1.9),
        "edge_w1": normal_values(keys[5], (LATENT, 3 * LATENT), (3 * LATENT) ** -0.5, 0.15625),
        "edge_b1": normal_values(keys[6], (LATENT,), 0.5, 3.0, (), jnp.float32),
        "edge_w2": normal_values(keys[7], (LATENT, LATENT), LATENT ** -0.5, 0.25),
        "message_gain": jnp.clip(1.0 + 0.18 * jax.random.normal(keys[8], (LATENT,), jnp.float32), 0.1, 1.9),
        "message_bias": normal_values(keys[9], (LATENT,), 0.5, 3.0, (), jnp.float32),
        "mesh_latent": normal_values(keys[10], (LATENT, BANDS, SECTORS, MESH_DEV), 1.0, 6.0, ((0, 4), (1, 4), (2, 2))),
        "edge_latent": normal_values(keys[11], (LATENT, BANDS, SECTORS, EDGE_DEV), 1.0, 6.0, ((0, 4), (1, 4), (2, 2))),
        "senders": draw_senders(jax.random.fold_in(keys[15], 71), 0),
        "receivers": draw_receivers(jax.random.fold_in(keys[15], 71), 0),
        "edge_counts": draw_edge_counts(jax.random.fold_in(keys[15], 71), 0),
    }


epsilon = 1e-05

def normalize(values):
    average = lax.optimization_barrier(jnp.mean(values, axis=0, keepdims=True))
    centred = values - average
    spread = lax.optimization_barrier(jnp.mean(centred * centred, axis=0, keepdims=True))
    return centred * lax.rsqrt(spread + epsilon)

def reference(grid_inputs, embed_w1, embed_b1, embed_w2, embed_gain, edge_w1, edge_b1, edge_w2, message_gain, message_bias, mesh_latent, edge_latent, senders, receivers, edge_counts):
    band_inputs = grid_inputs.reshape(CHANNELS, BANDS, GLAT * NLON).transpose(1, 0, 2)

    def embed_band(block_inputs):
        hidden = jax.nn.silu(jnp.dot(embed_w1, block_inputs, preferred_element_type=jnp.float32) + embed_b1[:, None]).astype(jnp.bfloat16)
        first_pre = jnp.dot(embed_w2, hidden, preferred_element_type=jnp.float32)
        return (normalize(first_pre) * embed_gain[:, None]).astype(jnp.bfloat16)
    band_latent = lax.map(embed_band, band_inputs)
    grid_latent = band_latent.transpose(1, 0, 2).reshape(LATENT, NLAT * NLON)
    tile_count = BANDS * SECTORS
    node_total = tile_count * MESH_DEV
    mesh_flat = mesh_latent.reshape(LATENT, node_total)
    edge_tiles = edge_latent.reshape(LATENT, tile_count, EDGE_DEV).transpose(1, 0, 2)
    send_tiles = senders.reshape(tile_count, EDGE_DEV)
    recv_tiles = receivers.reshape(tile_count, EDGE_DEV)
    count_tiles = edge_counts.reshape(tile_count)
    slot_ids = jnp.arange(EDGE_DEV, dtype=jnp.int32)

    def tile_step(running, inputs):
        totals, degree = running
        edge_cols, send_ids, recv_ids, live_count = inputs
        live_mask = slot_ids < live_count
        stacked = jnp.concatenate([edge_cols, jnp.take(grid_latent, send_ids, axis=1), jnp.take(mesh_flat, recv_ids, axis=1)], axis=0)
        hidden = jax.nn.silu(jnp.dot(edge_w1, stacked, preferred_element_type=jnp.float32) + edge_b1[:, None]).astype(jnp.bfloat16)
        second = jnp.dot(edge_w2, hidden, preferred_element_type=jnp.float32)
        message = (edge_cols.astype(jnp.float32) + normalize(second) * message_gain[:, None] + message_bias[:, None]).astype(jnp.bfloat16)
        weights = jnp.where(live_mask[None, :], message.astype(jnp.float32), jnp.float32(0.0))
        totals = totals + jax.ops.segment_sum(weights.T, recv_ids, num_segments=node_total)
        degree = degree + jax.ops.segment_sum(live_mask.astype(jnp.int32), recv_ids, num_segments=node_total)
        return ((totals, degree), None)
    start_state = (jnp.zeros((node_total, LATENT), jnp.float32), jnp.zeros((node_total,), jnp.int32))
    (totals, degree), unused = lax.scan(tile_step, start_state, (edge_tiles, send_tiles, recv_tiles, count_tiles))
    scale = jnp.maximum(degree, 1).astype(jnp.float32)
    result = mesh_flat.astype(jnp.float32) + totals.T / scale[None, :]
    mesh_out = result.astype(jnp.bfloat16).reshape(LATENT, BANDS, SECTORS, MESH_DEV)
    return (mesh_out, grid_latent.reshape(LATENT, NLAT, NLON))
```

```python
import functools

import jax
import jax.numpy as jnp
from jax import lax
from jax.experimental import pallas as pl
from jax.experimental.pallas import tpu as pltpu
from jax.sharding import PartitionSpec as P

HALO = 8
ROWS = 16
GROUP = 4

epsilon = 1e-05
F32 = jnp.float32
BF16 = jnp.bfloat16


def shifts(axis):
    size = lax.axis_size(axis)
    up = [(i, (i + 1) % size) for i in range(size)]
    return up, [(j, i) for i, j in up]


def half_silu(half):
    return half + half * jnp.tanh(half)


def centre(values):
    average = jnp.mean(values, axis=0, keepdims=True)
    centred = values - average
    spread = jnp.mean(centred * centred, axis=0, keepdims=True)
    return average, lax.rsqrt(spread + epsilon)


def onehot_of(index_row, first, count):
    ids = lax.broadcasted_iota(jnp.int32, (count, index_row.shape[1]), 0)
    return jnp.where(ids == index_row - first, 1.0, 0.0).astype(BF16)


def embed_kernel(step0, place_ref, x_ref, w1_ref, b1_ref, w2_ref, gain_ref, own_ref, *rest):
    out_ref, gathered_ref, wide, pre_ref, out_wide = rest[-5:]
    channels, rows, lon = x_ref.shape
    padded = w1_ref.shape[1]
    shard = out_ref.shape[0]
    step = pl.program_id(0)

    @pl.when(step == 0)
    def _():
        wide[pl.ds(channels * rows, (padded - channels) * rows), :] = jnp.zeros(
            ((padded - channels) * rows, lon), F32
        )
        if len(rest) == 5:
            gathered_ref[...] = jnp.zeros_like(gathered_ref)
        else:
            gathered_ref[...] = rest[1][...]

    wide[pl.ds(0, channels * rows), :] = x_ref[...].astype(F32).reshape(channels * rows, lon)
    gain = gain_ref[pl.ds(pl.multiple_of(place_ref[0] * shard, shard), shard), :]
    for group in range(rows // GROUP):
        cells = jnp.concatenate(
            [wide[pl.ds(group * GROUP + r, padded, stride=rows), :] for r in range(GROUP)], axis=1
        ).astype(BF16)
        half = jnp.dot(w1_ref[...], cells, preferred_element_type=F32) + b1_ref[...]
        hidden = half_silu(half).astype(BF16)
        pre_ref[...] = jnp.dot(w2_ref[...], hidden, preferred_element_type=F32)
        average, scale = centre(pre_ref[...])
        own = pre_ref[pl.ds(pl.multiple_of(place_ref[0] * shard, shard), shard), :]
        own = (own - average) * scale * gain
        for r in range(GROUP):
            out_wide[pl.ds(group * GROUP + r, shard, stride=rows), :] = own[:, r * lon : (r + 1) * lon]
        first = ((step0 + step) * rows + group * GROUP) * lon
        pick = onehot_of(own_ref[...], first, GROUP * lon)
        gathered_ref[...] += jnp.dot(cells, pick, preferred_element_type=F32)
    out_ref[...] = out_wide[...].reshape(shard, rows, lon).astype(BF16)


def embed(place, inputs, w1, b1, w2, gain, own_index, shard, start, stop, earlier):
    channels, lat, lon = inputs.shape
    latent, padded = w1.shape
    edges = own_index.shape[1]
    steps = (stop - start) // ROWS
    step0 = start // ROWS
    full = lambda a: pl.BlockSpec(a.shape, lambda i: (0,) * a.ndim)
    whole = (latent * padded + latent * latent + padded * edges) * (stop - start) * lon * 2
    return pl.pallas_call(
        functools.partial(embed_kernel, step0),
        grid=(steps,),
        in_specs=[
            pl.BlockSpec(memory_space=pltpu.SMEM),
            pl.BlockSpec((channels, ROWS, lon), lambda i: (0, i + step0, 0)),
            full(w1),
            full(b1),
            full(w2),
            full(gain),
            full(own_index),
        ]
        + ([pl.BlockSpec(memory_space=pl.ANY), full(earlier[1])] if earlier else []),
        out_specs=[
            pl.BlockSpec((shard, ROWS, lon), lambda i: (0, i + step0, 0)),
            pl.BlockSpec((padded, edges), lambda i: (0, 0)),
        ],
        out_shape=[
            jax.ShapeDtypeStruct((shard, lat, lon), BF16),
            jax.ShapeDtypeStruct((padded, edges), F32),
        ],
        scratch_shapes=[
            pltpu.VMEM((padded * ROWS, lon), F32),
            pltpu.VMEM((latent, GROUP * lon), F32),
            pltpu.VMEM((shard * ROWS, lon), F32),
        ],
        input_output_aliases={7: 0} if earlier else {},
        compiler_params=pltpu.CompilerParams(
            dimension_semantics=("arbitrary",), vmem_limit_bytes=40 * 1024 * 1024
        ),
        cost_estimate=pl.CostEstimate(
            flops=whole * 2, bytes_accessed=inputs.size + shard * lat * lon, transcendentals=0
        ),
    )(place, inputs, w1, b1, w2, gain, own_index, *(earlier or ()))


def edge_kernel(
    moved_ref, near_ref, send_ref, gathered_ref, up_ref, down_ref, left_ref, right_ref,
    w1_ref, b1_ref, w2_ref, gain_ref, e1_ref, eb1_ref, e2_ref, mgain_ref, mbias_ref,
    totals_ref, degree_ref,
):
    latent = w2_ref.shape[0]
    edges = send_ref.shape[1]
    slots = near_ref.shape[1]
    nodes = totals_ref.shape[1]
    picked = gathered_ref[...].astype(BF16).astype(F32)[: up_ref.shape[0]]
    first = 0
    for strip in (up_ref, down_ref, left_ref, right_ref):
        count = strip.shape[1]
        pick = onehot_of(send_ref[1:2, :], first, count)
        picked = picked + jnp.dot(strip[...], pick, preferred_element_type=F32)
        first += count
    picked = picked.astype(BF16)
    half = jnp.dot(w1_ref[...], picked, preferred_element_type=F32) + b1_ref[...]
    pre = jnp.dot(w2_ref[...], half_silu(half).astype(BF16), preferred_element_type=F32)
    average, scale = centre(pre)
    sender = ((pre - average) * scale * gain_ref[...]).astype(BF16)
    assigned = moved_ref[:, :edges]
    onehot = onehot_of(send_ref[2:3, :], 0, nodes)
    mesh_cols = jnp.dot(moved_ref[:, edges:], onehot, preferred_element_type=F32).astype(BF16)
    half = jnp.dot(e1_ref[:, :latent], assigned, preferred_element_type=F32)
    half = half + jnp.dot(e1_ref[:, latent : 2 * latent], sender, preferred_element_type=F32)
    half = half + jnp.dot(e1_ref[:, 2 * latent :], mesh_cols, preferred_element_type=F32)
    hidden = half_silu(half + eb1_ref[...]).astype(BF16)
    second = jnp.dot(e2_ref[...], hidden, preferred_element_type=F32)
    average, scale = centre(second)
    message = (
        assigned.astype(F32) + (second - average) * scale * mgain_ref[...] + mbias_ref[...]
    ).astype(BF16)
    last = (((1,), (1,)), ((), ()))
    totals_ref[...] = lax.dot_general(message, onehot, last, preferred_element_type=F32)
    degree = jnp.zeros(degree_ref.shape, F32)
    for start in range(0, slots, edges):
        chunk = onehot_of(near_ref[:, start : start + edges], 0, nodes)
        ones = jnp.ones((degree_ref.shape[0], edges), BF16)
        degree = degree + lax.dot_general(ones, chunk, last, preferred_element_type=F32)
    degree_ref[...] = jnp.maximum(degree, 1.0)


def edge_network(nodes, operands, latent):
    return pl.pallas_call(
        edge_kernel,
        out_shape=[
            jax.ShapeDtypeStruct((latent, nodes), F32),
            jax.ShapeDtypeStruct((8, nodes), F32),
        ],
        compiler_params=pltpu.CompilerParams(vmem_limit_bytes=48 * 1024 * 1024),
        cost_estimate=pl.CostEstimate(
            flops=4_000_000_000, bytes_accessed=8_000_000, transcendentals=0
        ),
    )(*operands)


def on_device(
    grid_inputs,
    embed_w1,
    embed_b1,
    embed_w2,
    embed_gain,
    edge_w1,
    edge_b1,
    edge_w2,
    message_gain,
    message_bias,
    mesh_latent,
    edge_latent,
    senders,
    receivers,
    edge_counts,
):
    latent = embed_w2.shape[0]
    channels, lat, lon = grid_inputs.shape
    shard = mesh_latent.shape[0]
    nodes = mesh_latent.shape[3]
    slots = edge_latent.shape[3]
    layers = lax.axis_size("gz")
    layer = lax.axis_index("gz")
    band = lax.axis_index("gx")
    sector = lax.axis_index("gy")
    lon_total = lon * lax.axis_size("gy")
    share = slots // layers
    padded = -(-channels // 16) * 16

    mesh_own = mesh_latent[:, 0, 0, :]
    edge_own = edge_latent[:, 0, 0, :].reshape(shard, layers, share).transpose(1, 0, 2)
    outgoing = jnp.concatenate(
        [edge_own, jnp.broadcast_to(mesh_own[None], (layers, shard, nodes))], axis=2
    )
    moved = lax.all_to_all(outgoing, "gz", split_axis=0, concat_axis=0, tiled=True)
    moved = moved.reshape(latent, share + nodes)

    up, down = shifts("gx")
    before = lax.ppermute(grid_inputs[:, lat - HALO :, :], "gx", up)
    after = lax.ppermute(grid_inputs[:, :HALO, :], "gx", down)

    slot_ids = jnp.arange(slots, dtype=jnp.int32)
    tile = band * lax.axis_size("gy") + sector
    near = jnp.where(slot_ids < edge_counts[0, 0], receivers[0, 0] - tile * nodes, -1)
    my_near = lax.dynamic_slice_in_dim(near, layer * share, share)
    send = lax.dynamic_slice_in_dim(senders[0, 0], layer * share, share)
    row = send // lon_total - band * lat
    column = (send % lon_total - sector * lon + HALO + lon_total) % lon_total - HALO
    inside_row = (row >= 0) & (row < lat)
    inside_column = (column >= 0) & (column < lon)
    own_index = jnp.where(inside_row & inside_column, row * lon + column, -1)
    strip = HALO * lon
    tall = (lat + 2 * HALO) * HALO
    row_index = jnp.where(row < 0, (row + HALO) * lon, strip + (row - lat) * lon) + column
    column_index = (
        jnp.where(column < 0, column + HALO, tall + column - lon) + 2 * strip + (row + HALO) * HALO
    )
    halo_index = jnp.where(
        inside_column, jnp.where(inside_row, -1, row_index), column_index
    )
    send_table = jnp.stack([own_index, halo_index, my_near])

    pad = lambda w: jnp.pad(w, ((0, 0), (0, padded - channels)))
    half_w1 = embed_w1 * 0.5
    half_b1 = (embed_b1 * 0.5)[:, None]
    gain = embed_gain[:, None]
    place = layer.reshape(1).astype(jnp.int32)
    middle = lat // 2 // ROWS * ROWS
    common = (place, grid_inputs, pad(half_w1), half_b1, embed_w2, gain, send_table[:1], shard)
    partial = embed(*common, 0, middle, None)

    left_cols = jnp.concatenate([a[:, :, :HALO] for a in (before, grid_inputs, after)], axis=1)
    right_cols = jnp.concatenate(
        [a[:, :, lon - HALO :] for a in (before, grid_inputs, after)], axis=1
    )
    up, down = shifts("gy")
    left = lax.ppermute(right_cols.reshape(channels, tall), "gy", up)
    right = lax.ppermute(left_cols.reshape(channels, tall), "gy", down)
    grid_out, gathered = embed(*common, middle, lat, partial)

    totals, degree = edge_network(
        nodes,
        (
            moved, near[None], send_table, gathered,
            before.reshape(channels, strip), after.reshape(channels, strip), left, right,
            half_w1, half_b1, embed_w2, gain,
            edge_w1 * 0.5, (edge_b1 * 0.5)[:, None], edge_w2,
            message_gain[:, None], message_bias[:, None],
        ),
        latent,
    )
    parts = lax.all_to_all(
        totals.reshape(layers, shard, nodes), "gz", split_axis=0, concat_axis=0, tiled=True
    )
    result = mesh_own.astype(F32) + jnp.sum(parts, axis=0) / degree[:1]
    return (result.astype(BF16).reshape(shard, 1, 1, nodes), grid_out)


def solution(mesh):
    return jax.shard_map(
        on_device,
        mesh=mesh,
        in_specs=(
            P(None, "gx", "gy"),
            P(),
            P(),
            P(),
            P(),
            P(),
            P(),
            P(),
            P(),
            P(),
            P("gz", "gx", "gy", None),
            P("gz", "gx", "gy", None),
            P("gx", "gy", None),
            P("gx", "gy", None),
            P("gx", "gy"),
        ),
        out_specs=(P("gz", "gx", "gy", None), P("gz", "gx", "gy")),
        check_vma=False,
    )
```

```python
import jax
import jax.numpy as jnp
from jax import lax
from jax.experimental import pallas as pl
from jax.experimental.pallas import tpu as pltpu
from jax.sharding import PartitionSpec as P

HALO = 8
ROWS = 16
GROUP = 4

epsilon = 1e-05
F32 = jnp.float32
BF16 = jnp.bfloat16


def half_silu(half):
    return half + half * jnp.tanh(half)


def centre(values):
    average = jnp.mean(values, axis=0, keepdims=True)
    centred = values - average
    spread = jnp.mean(centred * centred, axis=0, keepdims=True)
    return average, lax.rsqrt(spread + epsilon)


def onehot_of(index_row, first, count):
    ids = lax.broadcasted_iota(jnp.int32, (count, index_row.shape[1]), 0)
    return jnp.where(ids == index_row - first, 1.0, 0.0).astype(BF16)


MESH = pl.DeviceIdType.MESH


def partner(dx, dy, dz):
    ids = {}
    for axis, step in (("gx", dx), ("gy", dy), ("gz", dz)):
        size = lax.axis_size(axis)
        ids[axis] = lax.rem(lax.axis_index(axis) + (step + size), size)
    return ids


def kernel(
    x_hbm, w1_ref, w2_ref, e1_ref, e2_ref, vec_ref, mesh_ref, edge_ref, near_ref, send_ref,
    out_hbm, mesh_out_ref,
    x_ref, wide, w1, cols, gathered, pre_ref, out_wide, stage,
    rows_send, cols_send, rows_recv, cols_recv, corner_recv,
    assigned, nodes_all, totals, parts,
    x_sem, out_sem, halo_send, halo_recv, z_send, z_recv,
):
    tiles, channels, rows, lon = x_ref.shape
    padded = w1.shape[1]
    latent, share = assigned.shape
    shard, nodes = mesh_ref.shape
    slots = edge_ref.shape[1]
    layers = slots // share
    me = lax.axis_index("gz")
    mine = pl.ds(pl.multiple_of(me * shard, shard), shard)

    diagonals = ((1, 1), (1, -1), (-1, 1), (-1, -1))
    around = [(1, 0, 0), (-1, 0, 0), (0, 1, 0), (0, -1, 0)]
    around += [(dx, dy, 0) for dx, dy in diagonals]
    around += [(0, 0, k) for k in range(1, layers)]
    barrier = pltpu.get_barrier_semaphore()
    for offset in around:
        pl.semaphore_signal(barrier, inc=1, device_id=partner(*offset), device_id_type=MESH)
    loads = [
        pltpu.make_async_copy(x_hbm.at[:, pl.ds(t * rows, rows), :], x_ref.at[t], x_sem.at[t])
        for t in range(tiles)
    ]
    for load in loads:
        load.start()

    w1[...] = jnp.zeros_like(w1)
    w1[:, :channels] = w1_ref[...] * 0.5
    cols[...] = vec_ref[...].T
    b1, gain = cols[:, 0:1] * 0.5, cols[:, 1:2]
    gathered[...] = jnp.zeros_like(gathered)
    assigned[mine, :] = edge_ref[:, pl.ds(pl.multiple_of(me * share, share), share)]
    nodes_all[mine, :] = mesh_ref[...]
    pl.semaphore_wait(barrier, len(around))

    def remote(source, target, send_sem, recv_sem, offset):
        return pltpu.make_async_remote_copy(
            src_ref=source, dst_ref=target, send_sem=send_sem, recv_sem=recv_sem,
            device_id=partner(*offset), device_id_type=MESH,
        )

    spread = []
    for k in range(1, layers):
        peer = lax.rem(me + k, layers)
        theirs = pl.ds(pl.multiple_of(peer * share, share), share)
        spread.append(
            remote(edge_ref.at[:, theirs], assigned.at[mine, :], z_send.at[0, k], z_recv.at[0, k], (0, 0, k))
        )
        spread.append(
            remote(mesh_ref, nodes_all.at[mine, :], z_send.at[1, k], z_recv.at[1, k], (0, 0, k))
        )
    for copy in spread:
        copy.start()

    def widen(t, carry):
        wide[t, pl.ds(0, channels * rows), :] = x_ref[t].astype(F32).reshape(channels * rows, lon)
        wide[t, pl.ds(channels * rows, (padded - channels) * rows), :] = jnp.zeros(
            ((padded - channels) * rows, lon), F32
        )
        lanes = lax.broadcasted_iota(jnp.int32, (padded, lon), 1) // HALO
        left = jnp.zeros((padded, lon), F32)
        right = jnp.zeros((padded, lon), F32)
        for j in range(rows):
            row = wide[t, pl.ds(j, padded, stride=rows), :]
            here = lanes == j
            left = jnp.where(here, row if j == 0 else pltpu.roll(row, j * HALO, 1), left)
            turn = (j * HALO + HALO) % lon
            right = jnp.where(here, row if turn == 0 else pltpu.roll(row, turn, 1), right)
        cols_send[0, t] = left.astype(BF16)
        cols_send[1, t] = right.astype(BF16)
        return carry

    for load in loads:
        load.wait()
    lax.fori_loop(0, tiles, widen, 0)
    for j in range(HALO):
        at = pl.ds(j * lon, lon)
        rows_send[0, :, at] = wide[0, pl.ds(j, padded, stride=rows), :].astype(BF16)
        rows_send[1, :, at] = wide[
            tiles - 1, pl.ds(rows - HALO + j, padded, stride=rows), :
        ].astype(BF16)

    def embed(t):
        slot = 0
        own_gain = cols[mine, 1:2]
        for group in range(rows // GROUP):
            cells = jnp.concatenate(
                [wide[t, pl.ds(group * GROUP + r, padded, stride=rows), :] for r in range(GROUP)],
                axis=1,
            ).astype(BF16)
            half = jnp.dot(w1[...], cells, preferred_element_type=F32) + b1
            hidden = half_silu(half).astype(BF16)
            slot = group % 2
            pre_ref[slot] = jnp.dot(w2_ref[...], hidden, preferred_element_type=F32)
            average, scale = centre(pre_ref[slot])
            own = (pre_ref[slot, mine, :] - average) * scale * own_gain
            for r in range(GROUP):
                out_wide[pl.ds(group * GROUP + r, shard, stride=rows), :] = own[
                    :, r * lon : (r + 1) * lon
                ]
            first = (t * rows + group * GROUP) * lon
            pick = onehot_of(send_ref[0:1, :], first, GROUP * lon)
            gathered[...] += jnp.dot(cells, pick, preferred_element_type=F32)
        stage[t] = out_wide[...].reshape(shard, rows, lon).astype(BF16)

    def store(t):
        return pltpu.make_async_copy(
            stage.at[t], out_hbm.at[:, pl.ds(t * rows, rows), :], out_sem.at[t]
        )

    halo = [
        remote(rows_send.at[1], rows_recv.at[0], halo_send.at[0], halo_recv.at[0], (1, 0, 0)),
        remote(rows_send.at[0], rows_recv.at[1], halo_send.at[1], halo_recv.at[1], (-1, 0, 0)),
        remote(cols_send.at[1], cols_recv.at[0], halo_send.at[2], halo_recv.at[2], (0, 1, 0)),
        remote(cols_send.at[0], cols_recv.at[1], halo_send.at[3], halo_recv.at[3], (0, -1, 0)),
    ]
    for i, (dx, dy) in enumerate(diagonals):
        halo.append(
            remote(
                cols_send.at[1 if dy > 0 else 0, tiles - 1 if dx > 0 else 0],
                corner_recv.at[i], halo_send.at[4 + i], halo_recv.at[4 + i], (dx, dy, 0),
            )
        )
    for copy in halo:
        copy.start()

    def advance(t, carry):
        embed(t)
        store(t).start()
        return carry

    lax.fori_loop(0, tiles, advance, 0)

    for copy in halo:
        copy.wait()
    picked = gathered[...]
    first = 0
    pieces = [rows_recv[0], rows_recv[1]]
    pieces += [cols_recv[side, t] for side in range(2) for t in range(tiles)]
    pieces += [corner_recv[i] for i in range(4)]
    for piece in pieces:
        pick = onehot_of(send_ref[1:2, :], first, piece.shape[1])
        picked = picked + jnp.dot(piece, pick, preferred_element_type=F32)
        first += piece.shape[1]
    half = jnp.dot(w1[...], picked.astype(BF16), preferred_element_type=F32) + b1
    pre = jnp.dot(w2_ref[...], half_silu(half).astype(BF16), preferred_element_type=F32)
    average, scale = centre(pre)
    sender = ((pre - average) * scale * gain).astype(BF16)
    for copy in spread:
        copy.wait()
    onehot = onehot_of(send_ref[2:3, :], 0, nodes)
    mesh_cols = jnp.dot(nodes_all[...], onehot, preferred_element_type=F32).astype(BF16)
    half = jnp.dot(e1_ref[:, :latent], assigned[...], preferred_element_type=F32)
    half = half + jnp.dot(e1_ref[:, latent : 2 * latent], sender, preferred_element_type=F32)
    half = half + jnp.dot(e1_ref[:, 2 * latent :], mesh_cols, preferred_element_type=F32)
    hidden = half_silu((half + cols[:, 2:3]) * 0.5).astype(BF16)
    second = jnp.dot(e2_ref[...], hidden, preferred_element_type=F32)
    average, scale = centre(second)
    message = (
        assigned[...].astype(F32) + (second - average) * scale * cols[:, 3:4] + cols[:, 4:5]
    ).astype(BF16)
    last = (((1,), (1,)), ((), ()))
    totals[...] = lax.dot_general(message, onehot, last, preferred_element_type=F32)
    parts[0] = totals[mine, :]
    exchange = []
    for k in range(1, layers):
        peer = lax.rem(me + k, layers)
        theirs = pl.ds(pl.multiple_of(peer * shard, shard), shard)
        exchange.append(
            remote(totals.at[theirs, :], parts.at[k], z_send.at[2, k], z_recv.at[2, k], (0, 0, k))
        )
    for copy in exchange:
        copy.start()
    degree = jnp.zeros((8, nodes), F32)
    for start in range(0, slots, share):
        chunk = onehot_of(near_ref[:, start : start + share], 0, nodes)
        ones = jnp.ones((8, share), BF16)
        degree = degree + lax.dot_general(ones, chunk, last, preferred_element_type=F32)
    scale = jnp.maximum(degree[:1], 1.0)
    for copy in exchange:
        copy.wait()
    total = parts[0]
    for k in range(1, layers):
        total = total + parts[k]
    mesh_out_ref[...] = (mesh_ref[...].astype(F32) + total / scale).astype(BF16)
    for t in range(tiles):
        store(t).wait()


def on_device(
    grid_inputs,
    embed_w1,
    embed_b1,
    embed_w2,
    embed_gain,
    edge_w1,
    edge_b1,
    edge_w2,
    message_gain,
    message_bias,
    mesh_latent,
    edge_latent,
    senders,
    receivers,
    edge_counts,
):
    latent = embed_w2.shape[0]
    channels, lat, lon = grid_inputs.shape
    shard = mesh_latent.shape[0]
    nodes = mesh_latent.shape[3]
    slots = edge_latent.shape[3]
    layers = lax.axis_size("gz")
    layer = lax.axis_index("gz")
    band = lax.axis_index("gx")
    sector = lax.axis_index("gy")
    lon_total = lon * lax.axis_size("gy")
    share = slots // layers
    padded = -(-channels // 16) * 16
    tiles = lat // ROWS

    slot_ids = jnp.arange(slots, dtype=jnp.int32)
    tile = band * lax.axis_size("gy") + sector
    near = jnp.where(slot_ids < edge_counts[0, 0], receivers[0, 0] - tile * nodes, -1)
    my_near = lax.dynamic_slice_in_dim(near, layer * share, share)
    send = lax.dynamic_slice_in_dim(senders[0, 0], layer * share, share)
    row = send // lon_total - band * lat
    column = (send % lon_total - sector * lon + HALO + lon_total) % lon_total - HALO
    above, below = row < 0, row >= lat
    west, east = column < 0, column >= lon
    inside_row = ~(above | below)
    inside_column = ~(west | east)
    own_index = jnp.where(inside_row & inside_column, row * lon + column, -1)
    strip = HALO * lon
    tall = lat * HALO
    row_index = jnp.where(above, row + HALO, row - lat + HALO) * lon + column
    beside = jnp.where(west, column + HALO, column - lon)
    column_index = 2 * strip + jnp.where(west, 0, tall) + row * HALO + beside
    corner = jnp.where(above, 0, 2) + jnp.where(west, 0, 1)
    corner_row = jnp.where(above, row + ROWS, row - lat)
    corner_index = 2 * (strip + tall) + (corner * ROWS + corner_row) * HALO + beside
    halo_index = jnp.where(
        inside_column,
        jnp.where(inside_row, -1, row_index),
        jnp.where(inside_row, column_index, corner_index),
    )
    send_table = jnp.stack([own_index, halo_index, my_near])
    empty = jnp.zeros_like(embed_b1)
    vectors = jnp.stack(
        [embed_b1, embed_gain, edge_b1, message_gain, message_bias, empty, empty, empty]
    )

    vmem = pl.BlockSpec(memory_space=pltpu.VMEM)
    hbm = pl.BlockSpec(memory_space=pl.ANY)
    scratch = [
        ((tiles, channels, ROWS, lon), BF16),
        ((tiles, padded * ROWS, lon), F32),
        ((latent, padded), BF16),
        ((latent, 8), F32),
        ((padded, share), F32),
        ((2, latent, GROUP * lon), F32),
        ((shard * ROWS, lon), F32),
        ((tiles, shard, ROWS, lon), BF16),
        ((2, padded, strip), BF16),
        ((2, tiles, padded, lon), BF16),
        ((2, padded, strip), BF16),
        ((2, tiles, padded, lon), BF16),
        ((4, padded, lon), BF16),
        ((latent, share), BF16),
        ((latent, nodes), BF16),
        ((latent, nodes), F32),
        ((layers, shard, nodes), F32),
    ]
    sems = [(tiles,), (tiles,), (8,), (8,), (3, layers), (3, layers)]
    grid_out, mesh_out = pl.pallas_call(
        kernel,
        in_specs=[hbm] + [vmem] * 9,
        out_specs=[hbm, vmem],
        out_shape=[
            jax.ShapeDtypeStruct((shard, lat, lon), BF16),
            jax.ShapeDtypeStruct((shard, nodes), BF16),
        ],
        scratch_shapes=[pltpu.VMEM(s, d) for s, d in scratch]
        + [pltpu.SemaphoreType.DMA(s) for s in sems],
        compiler_params=pltpu.CompilerParams(
            collective_id=0, has_side_effects=True, vmem_limit_bytes=60 * 1024 * 1024
        ),
    )(
        grid_inputs, embed_w1, embed_w2, edge_w1, edge_w2, vectors,
        mesh_latent[:, 0, 0, :], edge_latent[:, 0, 0, :], near[None], send_table,
    )
    return (mesh_out.reshape(shard, 1, 1, nodes), grid_out)


def solution(mesh):
    return jax.shard_map(
        on_device,
        mesh=mesh,
        in_specs=(
            P(None, "gx", "gy"),
            P(),
            P(),
            P(),
            P(),
            P(),
            P(),
            P(),
            P(),
            P(),
            P("gz", "gx", "gy", None),
            P("gz", "gx", "gy", None),
            P("gx", "gy", None),
            P("gx", "gy", None),
            P("gx", "gy"),
        ),
        out_specs=(P("gz", "gx", "gy", None), P("gz", "gx", "gy")),
        check_vma=False,
    )
```

```python
import jax
import jax.numpy as jnp
from jax import lax
from jax.experimental import pallas as pl
from jax.experimental.pallas import tpu as pltpu
from jax.sharding import PartitionSpec as P

HALO = 8
ROWS = 16
GROUP = 4

epsilon = 1e-05
F32 = jnp.float32
BF16 = jnp.bfloat16


def half_silu(half):
    return half + half * jnp.tanh(half)


def centre(values):
    average = jnp.mean(values, axis=0, keepdims=True)
    centred = values - average
    spread = jnp.mean(centred * centred, axis=0, keepdims=True)
    return average, lax.rsqrt(spread + epsilon)


def onehot_of(index_row, first, count):
    ids = lax.broadcasted_iota(jnp.int32, (count, index_row.shape[1]), 0)
    return jnp.where(ids == index_row - first, 1.0, 0.0).astype(BF16)


MESH = pl.DeviceIdType.MESH


def partner(dx, dy, dz):
    ids = {}
    for axis, step in (("gx", dx), ("gy", dy), ("gz", dz)):
        size = lax.axis_size(axis)
        ids[axis] = lax.rem(lax.axis_index(axis) + (step + size), size)
    return ids


def split(values, size):
    if size & (size - 1) == 0:
        return lax.shift_right_logical(values, size.bit_length() - 1), values & (size - 1)
    return values // size, values % size


def locate(send, receive, live, near_ref, send_ref, nodes, lat, lon):
    band = lax.axis_index("gx")
    sector = lax.axis_index("gy")
    lon_total = lon * lax.axis_size("gy")
    slot_ids = lax.broadcasted_iota(jnp.int32, receive.shape, 1)
    tile = band * lax.axis_size("gy") + sector
    near_ref[...] = jnp.where(slot_ids < live, receive - tile * nodes, -1)
    row, column = split(send, lon_total)
    row = row - band * lat
    column = split(column - sector * lon + (HALO + lon_total), lon_total)[1] - HALO
    above, below = row < 0, row >= lat
    west, east = column < 0, column >= lon
    outside_row = jnp.where(above, 1, jnp.where(below, 1, 0))
    outside_column = jnp.where(west, 1, jnp.where(east, 1, 0))
    send_ref[0:1, :] = jnp.where(outside_row + outside_column == 0, row * lon + column, -1)
    strip = HALO * lon
    tall = lat * HALO
    row_index = jnp.where(above, row + HALO, row - lat + HALO) * lon + column
    beside = jnp.where(west, column + HALO, column - lon)
    column_index = 2 * strip + jnp.where(west, 0, tall) + row * HALO + beside
    corner = jnp.where(above, 0, 2) + jnp.where(west, 0, 1)
    corner_row = jnp.where(above, row + ROWS, row - lat)
    corner_index = 2 * (strip + tall) + (corner * ROWS + corner_row) * HALO + beside
    send_ref[1:2, :] = jnp.where(
        outside_column == 0,
        jnp.where(outside_row == 0, -1, row_index),
        jnp.where(outside_row == 0, column_index, corner_index),
    )


def kernel(
    x_hbm, w1_ref, w2_ref, e1_hbm, e2_hbm, b1_ref, gain_ref, eb1_ref, mgain_ref, mbias_ref,
    mesh_ref, edge_ref, senders_ref, receivers_ref, count_ref,
    out_hbm, mean_ref,
    x_ref, wide, w1, cols, e1_ref, e2_ref, w1_wide, vec_ref, near_ref, send_ref, gathered, pre_ref, out_wide, stage,
    rows_send, cols_send, rows_recv, cols_recv, corner_recv,
    assigned, nodes_all, totals, parts,
    x_sem, out_sem, w_sem, halo_send, halo_recv, z_send, z_recv,
):
    tiles, channels, rows, lon = x_ref.shape
    padded = w1.shape[1]
    latent, share = assigned.shape
    shard, nodes = mesh_ref.shape
    slots = edge_ref.shape[1]
    layers = slots // share
    me = lax.axis_index("gz")
    mine = pl.ds(pl.multiple_of(me * shard, shard), shard)

    diagonals = ((1, 1), (1, -1), (-1, 1), (-1, -1))
    around = [(1, 0, 0), (-1, 0, 0), (0, 1, 0), (0, -1, 0)]
    around += [(dx, dy, 0) for dx, dy in diagonals]
    around += [(0, 0, k) for k in range(1, layers)]
    barrier = pltpu.get_barrier_semaphore()
    for offset in around:
        pl.semaphore_signal(barrier, inc=1, device_id=partner(*offset), device_id_type=MESH)
    loads = [
        pltpu.make_async_copy(x_hbm.at[:, pl.ds(t * rows, rows), :], x_ref.at[t], x_sem.at[t])
        for t in range(tiles)
    ]
    weights = [
        pltpu.make_async_copy(e1_hbm, e1_ref, w_sem.at[0]),
        pltpu.make_async_copy(e2_hbm, e2_ref, w_sem.at[1]),
    ]
    for load in loads + weights:
        load.start()

    w1_wide[...] = jnp.zeros_like(w1_wide)
    w1_wide[:channels, :] = w1_ref[...].astype(F32) * 0.5
    w1[...] = w1_wide[...].T[:, :padded].astype(BF16)
    vec_ref[...] = jnp.zeros_like(vec_ref)
    for i, ref in enumerate((b1_ref, gain_ref, eb1_ref, mgain_ref, mbias_ref)):
        vec_ref[i : i + 1, :] = ref[...]
    cols[...] = vec_ref[...].T
    locate(
        senders_ref[:, pl.ds(pl.multiple_of(me * share, share), share)],
        receivers_ref[...], count_ref[0, 0], near_ref, send_ref, nodes, tiles * rows, lon,
    )
    send_ref[2:3, :] = near_ref[:, pl.ds(pl.multiple_of(me * share, share), share)]
    b1, gain = cols[:, 0:1] * 0.5, cols[:, 1:2]
    gathered[...] = jnp.zeros_like(gathered)
    assigned[mine, :] = edge_ref[:, pl.ds(pl.multiple_of(me * share, share), share)]
    nodes_all[mine, :] = mesh_ref[...]
    pl.semaphore_wait(barrier, len(around))

    def remote(source, target, send_sem, recv_sem, offset):
        return pltpu.make_async_remote_copy(
            src_ref=source, dst_ref=target, send_sem=send_sem, recv_sem=recv_sem,
            device_id=partner(*offset), device_id_type=MESH,
        )

    spread = []
    for k in range(1, layers):
        peer = lax.rem(me + k, layers)
        theirs = pl.ds(pl.multiple_of(peer * share, share), share)
        spread.append(
            remote(edge_ref.at[:, theirs], assigned.at[mine, :], z_send.at[0, k], z_recv.at[0, k], (0, 0, k))
        )
        spread.append(
            remote(mesh_ref, nodes_all.at[mine, :], z_send.at[1, k], z_recv.at[1, k], (0, 0, k))
        )
    for copy in spread:
        copy.start()

    def widen(t, carry):
        pltpu.make_async_copy(
            x_hbm.at[:, pl.ds(t * rows, rows), :], x_ref.at[t], x_sem.at[t]
        ).wait()
        wide[t, pl.ds(0, channels * rows), :] = x_ref[t].astype(F32).reshape(channels * rows, lon)
        wide[t, pl.ds(channels * rows, (padded - channels) * rows), :] = jnp.zeros(
            ((padded - channels) * rows, lon), F32
        )
        lanes = lax.broadcasted_iota(jnp.int32, (padded, lon), 1) // HALO
        left = jnp.zeros((padded, lon), F32)
        right = jnp.zeros((padded, lon), F32)
        for j in range(rows):
            row = wide[t, pl.ds(j, padded, stride=rows), :]
            here = lanes == j
            left = jnp.where(here, row if j == 0 else pltpu.roll(row, j * HALO, 1), left)
            turn = (j * HALO + HALO) % lon
            right = jnp.where(here, row if turn == 0 else pltpu.roll(row, turn, 1), right)
        cols_send[0, t] = left.astype(BF16)
        cols_send[1, t] = right.astype(BF16)
        return carry

    lax.fori_loop(0, tiles, widen, 0)
    for j in range(HALO):
        at = pl.ds(j * lon, lon)
        rows_send[0, :, at] = wide[0, pl.ds(j, padded, stride=rows), :].astype(BF16)
        rows_send[1, :, at] = wide[
            tiles - 1, pl.ds(rows - HALO + j, padded, stride=rows), :
        ].astype(BF16)

    def first_layer(t, group):
        cells = jnp.concatenate(
            [wide[t, pl.ds(group * GROUP + r, padded, stride=rows), :] for r in range(GROUP)],
            axis=1,
        ).astype(BF16)
        half = jnp.dot(w1[...], cells, preferred_element_type=F32) + b1
        return cells, half_silu(half).astype(BF16)

    def embed(t):
        own_gain = cols[mine, 1:2]
        cells, hidden = first_layer(t, 0)
        for group in range(rows // GROUP):
            slot = group % 2
            pre_ref[slot] = jnp.dot(w2_ref[...], hidden, preferred_element_type=F32)
            pick = onehot_of(send_ref[0:1, :], (t * rows + group * GROUP) * lon, GROUP * lon)
            gathered[...] += jnp.dot(cells, pick, preferred_element_type=F32)
            if (group + 1) * GROUP < rows:
                cells, hidden = first_layer(t, group + 1)
            average, scale = centre(pre_ref[slot])
            own = (pre_ref[slot, mine, :] - average) * scale * own_gain
            for r in range(GROUP):
                out_wide[pl.ds(group * GROUP + r, shard, stride=rows), :] = own[
                    :, r * lon : (r + 1) * lon
                ]
        stage[t] = out_wide[...].reshape(shard, rows, lon).astype(BF16)

    def store(t):
        return pltpu.make_async_copy(
            stage.at[t], out_hbm.at[:, pl.ds(t * rows, rows), :], out_sem.at[t]
        )

    halo = [
        remote(rows_send.at[1], rows_recv.at[0], halo_send.at[0], halo_recv.at[0], (1, 0, 0)),
        remote(rows_send.at[0], rows_recv.at[1], halo_send.at[1], halo_recv.at[1], (-1, 0, 0)),
        remote(cols_send.at[1], cols_recv.at[0], halo_send.at[2], halo_recv.at[2], (0, 1, 0)),
        remote(cols_send.at[0], cols_recv.at[1], halo_send.at[3], halo_recv.at[3], (0, -1, 0)),
    ]
    for i, (dx, dy) in enumerate(diagonals):
        halo.append(
            remote(
                cols_send.at[1 if dy > 0 else 0, tiles - 1 if dx > 0 else 0],
                corner_recv.at[i], halo_send.at[4 + i], halo_recv.at[4 + i], (dx, dy, 0),
            )
        )
    for copy in halo:
        copy.start()

    def advance(t, carry):
        embed(t)
        store(t).start()
        return carry

    lax.fori_loop(0, tiles, advance, 0)

    for copy in halo:
        copy.wait()
    picked = gathered[...]
    first = 0
    pieces = [rows_recv[0], rows_recv[1]]
    pieces += [cols_recv[side, t] for side in range(2) for t in range(tiles)]
    pieces += [corner_recv[i] for i in range(4)]
    for piece in pieces:
        pick = onehot_of(send_ref[1:2, :], first, piece.shape[1])
        picked = picked + jnp.dot(piece, pick, preferred_element_type=F32)
        first += piece.shape[1]
    half = jnp.dot(w1[...], picked.astype(BF16), preferred_element_type=F32) + b1
    pre = jnp.dot(w2_ref[...], half_silu(half).astype(BF16), preferred_element_type=F32)
    average, scale = centre(pre)
    sender = ((pre - average) * scale * gain).astype(BF16)
    for copy in spread:
        copy.wait()
    onehot = onehot_of(send_ref[2:3, :], 0, nodes)
    mesh_cols = jnp.dot(nodes_all[...], onehot, preferred_element_type=F32).astype(BF16)
    for copy in weights:
        copy.wait()
    half = jnp.dot(e1_ref[:, :latent], assigned[...], preferred_element_type=F32)
    half = half + jnp.dot(e1_ref[:, latent : 2 * latent], sender, preferred_element_type=F32)
    half = half + jnp.dot(e1_ref[:, 2 * latent :], mesh_cols, preferred_element_type=F32)
    hidden = half_silu((half + cols[:, 2:3]) * 0.5).astype(BF16)
    second = jnp.dot(e2_ref[...], hidden, preferred_element_type=F32)
    average, scale = centre(second)
    message = (
        assigned[...].astype(F32) + (second - average) * scale * cols[:, 3:4] + cols[:, 4:5]
    ).astype(BF16)
    last = (((1,), (1,)), ((), ()))
    totals[...] = lax.dot_general(message, onehot, last, preferred_element_type=F32)
    parts[0] = totals[mine, :]
    exchange = []
    for k in range(1, layers):
        peer = lax.rem(me + k, layers)
        theirs = pl.ds(pl.multiple_of(peer * shard, shard), shard)
        exchange.append(
            remote(totals.at[theirs, :], parts.at[k], z_send.at[2, k], z_recv.at[2, k], (0, 0, k))
        )
    for copy in exchange:
        copy.start()
    degree = jnp.zeros((8, nodes), F32)
    for start in range(0, slots, share):
        chunk = onehot_of(near_ref[:, start : start + share], 0, nodes)
        ones = jnp.ones((8, share), BF16)
        degree = degree + lax.dot_general(ones, chunk, last, preferred_element_type=F32)
    scale = jnp.maximum(degree[:1], 1.0)
    for copy in exchange:
        copy.wait()
    total = parts[0]
    for k in range(1, layers):
        total = total + parts[k]
    mean_ref[...] = total / scale
    for t in range(tiles):
        store(t).wait()


def on_device(
    grid_inputs,
    embed_w1,
    embed_b1,
    embed_w2,
    embed_gain,
    edge_w1,
    edge_b1,
    edge_w2,
    message_gain,
    message_bias,
    mesh_latent,
    edge_latent,
    senders,
    receivers,
    edge_counts,
):
    latent = embed_w2.shape[0]
    channels, lat, lon = grid_inputs.shape
    shard = mesh_latent.shape[0]
    nodes = mesh_latent.shape[3]
    slots = edge_latent.shape[3]
    layers = lax.axis_size("gz")
    share = slots // layers
    strip = HALO * lon
    padded = -(-channels // 16) * 16
    tiles = lat // ROWS

    vmem = pl.BlockSpec(memory_space=pltpu.VMEM)
    hbm = pl.BlockSpec(memory_space=pl.ANY)
    scratch = [
        ((tiles, channels, ROWS, lon), BF16),
        ((tiles, padded * ROWS, lon), F32),
        ((latent, padded), BF16),
        ((latent, 8), F32),
        (edge_w1.shape, BF16),
        (edge_w2.shape, BF16),
        ((-(-padded // 128) * 128, latent), F32),
        ((8, latent), F32),
        ((1, slots), jnp.int32),
        ((8, share), jnp.int32),
        ((padded, share), F32),
        ((2, latent, GROUP * lon), F32),
        ((shard * ROWS, lon), F32),
        ((tiles, shard, ROWS, lon), BF16),
        ((2, padded, strip), BF16),
        ((2, tiles, padded, lon), BF16),
        ((2, padded, strip), BF16),
        ((2, tiles, padded, lon), BF16),
        ((4, padded, lon), BF16),
        ((latent, share), BF16),
        ((latent, nodes), BF16),
        ((latent, nodes), F32),
        ((layers, shard, nodes), F32),
    ]
    sems = [(tiles,), (tiles,), (2,), (8,), (8,), (3, layers), (3, layers)]
    smem = pl.BlockSpec(memory_space=pltpu.SMEM)
    line = lambda v: v.reshape(1, v.size)
    mesh_own = mesh_latent[:, 0, 0, :]
    grid_out, mean = pl.pallas_call(
        kernel,
        in_specs=[hbm, vmem, vmem, hbm, hbm] + [vmem] * 9 + [smem],
        out_specs=[hbm, vmem],
        out_shape=[
            jax.ShapeDtypeStruct((shard, lat, lon), BF16),
            jax.ShapeDtypeStruct((shard, nodes), F32),
        ],
        scratch_shapes=[pltpu.VMEM(s, d) for s, d in scratch]
        + [pltpu.SemaphoreType.DMA(s) for s in sems],
        compiler_params=pltpu.CompilerParams(
            collective_id=0, has_side_effects=True, vmem_limit_bytes=60 * 1024 * 1024
        ),
    )(
        grid_inputs, embed_w1.T, embed_w2, edge_w1, edge_w2,
        line(embed_b1), line(embed_gain), line(edge_b1), line(message_gain), line(message_bias),
        mesh_own, edge_latent[:, 0, 0, :], line(senders), line(receivers), edge_counts,
    )
    mesh_out = (mesh_own.astype(F32) + mean).astype(BF16)
    return (mesh_out.reshape(shard, 1, 1, nodes), grid_out)


def solution(mesh):
    return jax.shard_map(
        on_device,
        mesh=mesh,
        in_specs=(
            P(None, "gx", "gy"),
            P(),
            P(),
            P(),
            P(),
            P(),
            P(),
            P(),
            P(),
            P(),
            P("gz", "gx", "gy", None),
            P("gz", "gx", "gy", None),
            P("gx", "gy", None),
            P("gx", "gy", None),
            P("gx", "gy"),
        ),
        out_specs=(P("gz", "gx", "gy", None), P("gz", "gx", "gy")),
        check_vma=False,
    )
```
